32 devices in a mesh: parts: 2 (over y), tok: 4 (over z), hid: 4 (over x, core).
Axes of the slice: x: 2, y: 2, z: 4, core: 2. Of those that a mesh axis runs over, the one named last changes fastest.
Arguments:
- tokens: bfloat16 [6144, 8192], P(('parts', 'tok'), 'hid'), parts along dimension 0, may hold values from -6 to 6
- adapter_ids: int32 [6144, 1], P(('parts', 'tok')), parts along dimension 0, may hold values from 0 to 31; in each aligned block of 768 rows (0 to 767, 768 to 1535, ...) at most 72 rows name the same one
- value_weight: bfloat16 [8192, 1024], P('hid'), may hold values from -0.0625 to 0.0625
- adapter_down: bfloat16 [32, 16, 8192], P('tok', None, 'hid'), may hold values from -0.0625 to 0.0625
- adapter_up: bfloat16 [32, 16, 1024], P('tok', None, 'hid'), may hold values from -1.5 to 1.5
Outputs:
- value_out: bfloat16 [6144, 1024], P(('parts', 'tok'), 'hid'), parts along dimension 0
The draws below stay inside these ranges and needn't reach their ends.
There are 2 independent parts, one for each index of `parts`. The reference program is written for one: setup_inputs(seed, part) draws one part's arguments, and reference() takes and returns one part's arrays. A program takes and returns all parts, laid end to end along the dimension named above; an argument that names none is the same for every part. Nothing has to cross between parts.
Inputs may be any that keep to these rules, and one draw needn't show every extreme that they name: `adapter_ids`: among the 768 tokens of one index of tok, each adapter id appears at most 72 times; in some of these aligned blocks one id appears exactly 72 times.
All inputs are finite; a program needn't handle non-finite values.
Results may differ from the reference program's by a relative error of at most 0.0048.
Values may be sent and summed in bfloat16 or wider, within the bound.
A program may use at most 128 MiB of HBM per device.

```python
import math
import jax
import jax.numpy as jnp
import numpy as np
from jax import lax

D = 8192
KV = 1024
R = 16
TOK_DEV = 768
ADAPTERS = 32
CAP = 72
TOKENS = 3072


def levels(own_key, dims, shards, smallest, high):
    gain, own = 1.0, jax.random.fold_in(own_key, 6)
    for position, shards_of in shards:
        steps = jnp.exp(jax.random.uniform(jax.random.fold_in(own, position), (shards_of,), jnp.float32, smallest / len(shards), high / len(shards)))
        gain = gain * jnp.repeat(steps, dims[position] // shards_of).reshape([-1 if axis == position else 1 for axis in range(len(dims))])
    return gain


def routed_block(key, own, number, rows, number_of, top, reach, lean):
    ranking = jax.random.permutation(key, number_of)
    heavy_load, common = portions_of(number_of, rows * top, reach, lean, True), portions_of(number_of, rows * top, reach, lean, False)
    places = jnp.arange(number_of)

    def named(tallies, offset_by):
        used = int((tallies > 0).sum())
        fixed = max(1, used // 4)
        moved = fixed + (places - fixed + offset_by * (used - fixed)) % max(1, number_of - fixed)
        return jnp.zeros((number_of,), jnp.int32).at[ranking[jnp.where(places < fixed, places, moved)]].set(jnp.asarray(tallies, jnp.int32))

    tallies = jnp.where(number % 4 == 0, named(heavy_load, number // 4), named(common, number - number // 4 - 1))
    mixed = jax.random.permutation(jax.random.fold_in(own, 3), number_of)
    source_of, receiver = mixed[0:number_of // 2 * 2:2], mixed[1:number_of // 2 * 2:2]
    slack = jnp.minimum(tallies[source_of] - 1, reach - tallies[receiver]) // 2
    slack = jnp.where((source_of == ranking[0]) | (receiver == ranking[0]) | (tallies[receiver] == 0), 0, jnp.maximum(slack, 0))
    moved = jax.random.randint(jax.random.fold_in(own, 4), (number_of // 2,), 0, 1 << 20) % (slack + 1)
    tallies = tallies.at[source_of].add(-moved).at[receiver].add(moved)
    labels = jnp.searchsorted(jnp.cumsum(tallies), jnp.arange(rows * top), side="right").astype(jnp.int32)
    listing = labels.reshape(top, rows).T
    listing = listing[jax.random.permutation(jax.random.fold_in(own, 1), rows)]
    offset_by = jax.random.randint(jax.random.fold_in(own, 2), (rows, 1), 0, top)
    return jnp.take_along_axis(listing, (jnp.arange(top)[None, :] + offset_by) % top, axis=1)


def portions_of(number_of, total, limit, slope, full):
    portions = [(1 << 20) // math.isqrt(grade ** slope) + 1 for grade in range(1, number_of + 1)]
    largest = limit if full else min(limit, max(-(-total // number_of), total * portions[0] // sum(portions)))
    least = 1 if total - largest >= number_of - 1 else 0
    holding, spare = [largest] + [least] * (number_of - 1), total - largest - least * (number_of - 1)
    while spare > 0:
        candidates = [i for i in range(1, number_of) if holding[i] < largest] or [i for i in range(1, number_of) if holding[i] < limit]
        mass, remaining = sum([portions[i] for i in candidates]), spare
        for i in candidates:
            extra = min(limit - holding[i], max(1, remaining * portions[i] // mass), spare)
            holding[i] = holding[i] + extra
            spare = spare - extra
    return np.array(holding)


def noise(key, extent, scale, most, cuts=(), held_as=jnp.bfloat16):
    result = scale * jax.random.normal(key, extent, jnp.float32)
    if cuts:
        result = result * levels(key, extent, cuts, -0.22, 0.18)
    return jnp.clip(result, -most, most).astype(held_as)


def setup_inputs(seed: int = 0, part: int = 0) -> dict:
    seeds = jax.random.split(jax.random.key(seed), 6)
    part_keys = jax.random.split(jax.random.fold_in(seeds[5], part), 6)
    tokens = noise(part_keys[0], (TOKENS, D), 1.0, 6.0, ((0, 4), (1, 4)))
    adapter_ids_keys = jax.random.split(jax.random.fold_in(part_keys[1], 1), TOKENS // TOK_DEV)
    adapter_ids_turns = jax.random.permutation(jax.random.fold_in(part_keys[1], 3), TOKENS // TOK_DEV)
    adapter_ids = jax.vmap(lambda own, number: routed_block(jax.random.fold_in(part_keys[1], 2), own, number, TOK_DEV, ADAPTERS, 1, CAP, 2))(adapter_ids_keys, adapter_ids_turns).reshape((TOKENS, 1))
    value_weight = noise(seeds[2], (D, KV), D ** -0.5, 0.0625, ((0, 4),))
    adapter_down = noise(seeds[3], (ADAPTERS, R, D), D ** -0.5, 0.0625, ((0, 4), (2, 4)))
    adapter_up = noise(seeds[4], (ADAPTERS, R, KV), R ** -0.5, 1.5, ((0, 4), (2, 4)))
    return {"tokens": tokens, "adapter_ids": adapter_ids, "value_weight": value_weight, "adapter_down": adapter_down, "adapter_up": adapter_up}


def reference(tokens, adapter_ids, value_weight, adapter_down, adapter_up):
    base_sums = jnp.dot(tokens, value_weight, preferred_element_type=jnp.float32)
    block_rows = math.gcd(TOKENS, 512)
    block_count = TOKENS // block_rows
    token_blocks = tokens.reshape(block_count, block_rows, D)
    id_blocks = adapter_ids[:, 0].reshape(block_count, block_rows)

    def block_delta(block_args):
        rows_block, ids_block = block_args
        down_picked = adapter_down[ids_block].astype(jnp.float32)
        low_rows = jnp.einsum("td,trd->tr", rows_block.astype(jnp.float32), down_picked).astype(jnp.bfloat16)
        up_picked = adapter_up[ids_block].astype(jnp.float32)
        return jnp.einsum("tr,trk->tk", low_rows.astype(jnp.float32), up_picked).astype(jnp.bfloat16)

    delta_rows = lax.map(block_delta, (token_blocks, id_blocks)).reshape(TOKENS, KV)
    return (base_sums + delta_rows.astype(jnp.float32)).astype(jnp.bfloat16)
```

```python
import functools

import jax
import jax.numpy as jnp
from jax import lax
from jax.experimental import pallas as pl
from jax.experimental.pallas import tpu as pltpu
from jax.sharding import PartitionSpec as P

MESH = pl.DeviceIdType.MESH
F32 = jnp.float32
BF16 = jnp.bfloat16

CHUNKS = 4
SPLIT = 2
PIECES = CHUNKS * SPLIT
EXTRA = SPLIT
UP = PIECES + EXTRA


def kernel(
    n_tok,
    n_hid,
    rank,
    ids_hbm,
    tokens_hbm,
    value_hbm,
    down_hbm,
    up_hbm,
    out_ref,
    ids,
    tokens,
    value,
    downs,
    ups,
    core_send,
    core_recv,
    partial,
    chip_send,
    chip_recv,
    picked,
    wanted,
    low_send,
    low_recv,
    load_sem,
    right_sem,
    left_sem,
    line_sem,
    extra_sem,
    pair_send_sem,
    pair_recv_sem,
    core_send_sem,
    core_recv_sem,
    chip_send_sem,
    chip_recv_sem,
    low_send_sem,
    low_recv_sem,
    ready_sem,
):
    y = lax.axis_index("parts")
    z = lax.axis_index("tok")
    h = lax.axis_index("hid")
    chips = n_hid // 2
    core = lax.rem(h, 2)
    x = lax.div(h, 2)
    rows, depth = tokens.shape
    kv = out_ref.shape[1]
    lanes, width = downs.shape[2:]
    adp_dev = lanes // rank
    part = lanes // SPLIT
    last = n_tok - 1

    load_down = [
        pltpu.make_async_copy(
            down_hbm.at[:, pl.ds(p * width, width)], downs.at[z, p], load_sem.at[3]
        )
        for p in range(2 * CHUNKS)
    ]
    chip_of = [lax.rem(x + d, chips) for d in range(chips)]
    order = [*range(1, chips), 0]
    columns_of = [(d, side) for d in order for side in (1, 0)]
    load_value = [
        pltpu.make_async_copy(
            value_hbm.at[
                :,
                pl.ds(
                    pl.multiple_of((chip_of[d] * 2 + (1 - core if side else core)) * kv, kv), kv
                ),
            ],
            value.at[k],
            load_sem.at[4],
        )
        for k, (d, side) in enumerate(columns_of)
    ]
    load_up = pltpu.make_async_copy(up_hbm, ups.at[z], load_sem.at[0])
    load_ids = pltpu.make_async_copy(ids_hbm, ids, load_sem.at[1])
    load_tokens = pltpu.make_async_copy(tokens_hbm, tokens, load_sem.at[2])
    for load in load_down:
        load.start()

    barrier = pltpu.get_barrier_semaphore()
    pl.semaphore_signal(barrier, inc=1, device_id={"parts": 1 - y}, device_id_type=MESH)
    for d in range(1, n_hid):
        pl.semaphore_signal(
            barrier, inc=1, device_id={"hid": lax.rem(h + d, n_hid)}, device_id_type=MESH
        )

    @pl.when(z < last)
    def _():
        pl.semaphore_signal(barrier, inc=1, device_id={"tok": z + 1}, device_id_type=MESH)

    pltpu.make_async_copy(downs.at[z], downs.at[z], load_sem.at[3]).wait()
    load_tokens.start()
    for load in load_value:
        load.start()
    load_up.start()
    load_ids.start()

    pl.semaphore_wait(barrier, n_hid + (z > 0).astype(jnp.int32))

    def piece(block, side, c):
        return downs.at[block, side * CHUNKS + c // SPLIT, pl.ds(c % SPLIT * part, part)]

    def line_piece(block, c):
        if c == UP:
            return ups.at[block]
        return piece(block, y, c) if c < PIECES else piece(block, 1 - y, c - EXTRA)

    def send_index(block, c):
        if c == UP:
            return n_tok + block
        return block if c < PIECES else 2 * n_tok

    def recv_sem(block, side, c):
        if PIECES <= c < UP:
            return extra_sem.at[side, c - PIECES]
        return line_sem.at[block - side, min(c, PIECES)]

    def to_right(block, c, ref=None):
        ref = line_piece(block, c) if ref is None else ref
        return pltpu.make_async_remote_copy(
            src_ref=ref,
            dst_ref=ref,
            send_sem=right_sem.at[send_index(block, c)],
            recv_sem=recv_sem(block, 0, c),
            device_id={"tok": z + 1},
            device_id_type=MESH,
        )

    def to_left(block, c, ref=None):
        ref = line_piece(block, c) if ref is None else ref
        return pltpu.make_async_remote_copy(
            src_ref=ref,
            dst_ref=ref,
            send_sem=left_sem.at[send_index(block, c)],
            recv_sem=recv_sem(block, 1, c),
            device_id={"tok": z - 1},
            device_id_type=MESH,
        )

    def to_pair(block, side, c, ref=None):
        ref = piece(block, side, c) if ref is None else ref
        return pltpu.make_async_remote_copy(
            src_ref=ref,
            dst_ref=ref,
            send_sem=pair_send_sem.at[block],
            recv_sem=pair_recv_sem.at[block - (block > z).astype(jnp.int32), c // SPLIT],
            device_id={"parts": 1 - y},
            device_id_type=MESH,
        )

    def wait_pair(block, c):
        @pl.when(by_pair(block, c * SPLIT))
        def _():
            ref = downs.at[block, (1 - y) * CHUNKS + c]
            to_pair(block, 1 - y, c * SPLIT, ref).wait_recv()

    @pl.when(z > 0)
    def _():
        pl.semaphore_signal(ready_sem, inc=1, device_id={"tok": z - 1}, device_id_type=MESH)
        for c in range(PIECES):
            to_left(z, c).start()

    @pl.when(z == last)
    def _():
        for c in range(PIECES, PIECES + EXTRA):
            to_left(z, c).start()

    def send_right():
        pl.semaphore_wait(ready_sem, 1)
        for c in range(PIECES):
            to_right(z, c).start()

        @pl.when(z == 0)
        def _():
            for c in range(PIECES, PIECES + EXTRA):
                to_right(z, c).start()

    def by_pair(block, c):
        return c < PIECES - EXTRA or (block != 0) & (block != last)

    def forward(s, first, end):
        from_left = z - 1 - s
        from_right = z + 1 + s
        for c in range(first, end):
            @pl.when(from_left >= 0 if c < PIECES else from_left == 0)
            def _():
                to_right(from_left, c).wait_recv()

                @pl.when(z < last)
                def _():
                    to_right(from_left, c).start()

                if c < PIECES:
                    @pl.when(by_pair(from_left, c))
                    def _():
                        to_pair(from_left, y, c).start()

            @pl.when(from_right <= last if c < PIECES else from_right == last)
            def _():
                to_left(from_right, c).wait_recv()

                @pl.when(z > 0)
                def _():
                    to_left(from_right, c).start()

                if c < PIECES:
                    @pl.when(by_pair(from_right, c))
                    def _():
                        to_pair(from_right, y, c).start()

    def forward_up(s):
        from_left = z - 1 - s
        from_right = z + 1 + s

        @pl.when((from_left >= 0) & (z < last))
        def _():
            to_right(from_left, UP).wait_recv()

            @pl.when((z < last - 1) | (s == n_tok - 3))
            def _():
                to_right(from_left, UP).start()

        @pl.when((from_right <= last) & (z > 0))
        def _():
            to_left(from_right, UP).wait_recv()

            @pl.when((z > 1) | (s == n_tok - 3))
            def _():
                to_left(from_right, UP).start()

    def flush_up():
        def send(block, carry):
            @pl.when(z == 1)
            def _():
                to_left(block, UP).start()

            @pl.when(z == last - 1)
            def _():
                to_right(block, UP).start()

            return carry

        lax.fori_loop(1, last, send, 0)

    alone = pl.when(z < n_tok)

    def base_block(k):
        return jnp.dot(tokens[...], value[k], preferred_element_type=F32)

    def to_core(d):
        return pltpu.make_async_remote_copy(
            src_ref=core_send.at[chip_of[d]],
            dst_ref=core_recv.at[chip_of[d]],
            send_sem=core_send_sem.at[d],
            recv_sem=core_recv_sem.at[d],
            device_id={"hid": x * 2 + 1 - core},
            device_id_type=MESH,
        )

    def to_chip(d, slot):
        i = chip_of[d]
        return pltpu.make_async_remote_copy(
            src_ref=chip_send.at[i],
            dst_ref=chip_recv.at[slot],
            send_sem=chip_send_sem.at[i],
            recv_sem=chip_recv_sem.at[slot],
            device_id={"hid": i * 2 + core},
            device_id_type=MESH,
        )

    pl.when((z > 0) & (z < last))(send_right)
    load_tokens.wait()
    pltpu.make_async_copy(value, value, load_sem.at[4]).wait()
    for n, d in enumerate(order):
        i = chip_of[d]

        @alone
        def _():
            core_send[i] = base_block(2 * n).astype(BF16)

        to_core(d).start()
        if n == 0:
            pl.when(z == 0)(send_right)
            load_up.wait()

            @pl.when(z > 1)
            def _():
                to_left(z, UP).start()

            @pl.when(z < last - 1)
            def _():
                to_right(z, UP).start()

        if d == 0:
            forward(0, 0, 1)

        @alone
        def _():
            partial[i] = base_block(2 * n + 1)

        if d > 0:
            to_core(d).wait_recv()
            chip_send[i] = (partial[i] + core_recv[i].astype(F32)).astype(BF16)
            to_chip(d, x).start()

    forward(0, 1, 3)

    load_ids.wait()
    lane_adapter = lax.broadcasted_iota(jnp.int32, (rows, lanes), 1) // rank
    ids_rows = jnp.transpose(jnp.broadcast_to(ids[...], (lanes, rows)))
    wanted[...] = ids_rows - lane_adapter

    def low_part(block, p):
        columns = pl.ds(pl.multiple_of(p * width, width), width)
        return lax.dot_general(
            tokens[:, columns],
            downs[block, p],
            (((1,), (1,)), ((), ())),
            preferred_element_type=F32,
        )

    def chosen_of(block, sums):
        return jnp.where(wanted[...] == block * adp_dev, sums, 0.0)

    def low_block(block):
        return lax.dot_general(
            tokens[...],
            jnp.concatenate([downs[block, p] for p in range(2 * CHUNKS)], axis=1),
            (((1,), (1,)), ((), ())),
            preferred_element_type=F32,
        )

    @alone
    def _():
        picked[...] = chosen_of(z, low_block(z))


    forward(0, 3, PIECES + EXTRA)

    def low_chunk(s, c):
        for at, block in ((last, last - 1 - s), (0, 1 + s)):
            @pl.when(z == at)
            def _():
                wait_pair(block, c)
                sums = low_part(block, y * CHUNKS + c) + low_part(block, (1 - y) * CHUNKS + c)
                picked[...] += chosen_of(block, sums)

    def low_whole(block, carry):
        @pl.when(block != z)
        def _():
            for c in range(CHUNKS):
                wait_pair(block, c)

            picked[...] += chosen_of(block, low_block(block))

        return carry

    def step(s, carry=0):
        for c in range(CHUNKS):
            forward(s, c * SPLIT, (c + 1) * SPLIT)
            if c == 1:
                forward_up(s - 1)
            low_chunk(s - 1, c)
        forward(s, PIECES, PIECES + EXTRA)
        return carry

    if n_tok <= 8:
        for s in range(1, n_tok - 2):
            step(s)
    else:
        lax.fori_loop(1, n_tok - 2, step, 0)
    flush_up()

    s = n_tok - 2
    for c in range(CHUNKS):
        forward(s, c * SPLIT, (c + 1) * SPLIT)
        if c == 1:
            forward_up(s - 1)
        if c < CHUNKS - 1:
            low_chunk(s - 1, c)
        if c == CHUNKS - 2:
            low_chunk(s - 1, CHUNKS - 1)
    low_chunk(s, 0)

    to_core(0).wait_recv()
    total = partial[x] + core_recv[x].astype(F32)
    for d in range(1, chips):
        to_chip(d, chip_of[d]).wait_recv()
        total += chip_recv[chip_of[d]].astype(F32)
    partial[x] = total

    forward(s, PIECES, PIECES + EXTRA)
    for c in range(1, CHUNKS - 2):
        low_chunk(s, c)
    low_chunk(s, CHUNKS - 1)
    low_chunk(s, CHUNKS - 2)

    @pl.when((z > 0) & (z < last))
    def _():
        lax.fori_loop(0, n_tok, low_whole, 0)

    fold = (
        lax.rem(lax.broadcasted_iota(jnp.int32, (rank, lanes), 1), rank)
        == lax.broadcasted_iota(jnp.int32, (rank, lanes), 0)
    ).astype(F32).astype(BF16)
    low_send[...] = lax.dot_general(
        fold,
        picked[...].astype(BF16),
        (((1,), (1,)), ((), ())),
        preferred_element_type=F32,
    ).astype(BF16)

    def to_hid(d, slot, ref=None):
        return pltpu.make_async_remote_copy(
            src_ref=low_send if ref is None else ref,
            dst_ref=low_recv.at[slot] if ref is None else ref,
            send_sem=low_send_sem,
            recv_sem=low_recv_sem.at[slot],
            device_id={"hid": lax.rem(h + d, n_hid)},
            device_id_type=MESH,
        )

    for d in range(1, n_hid):
        to_hid(d, h).start()

    def late_up(block, carry):
        @pl.when((z == 0) & (block > 0))
        def _():
            to_left(block, UP).wait_recv()

        @pl.when((z == last) & (block < last))
        def _():
            to_right(block, UP).wait_recv()

        return carry

    lax.fori_loop(0, n_tok, late_up, 0)

    low = low_send[...].astype(F32)
    for d in range(1, n_hid):
        slot = lax.rem(h + d, n_hid)
        to_hid(d, slot).wait_recv()
        low += low_recv[slot].astype(F32)
    low = low.astype(BF16)

    spread = lax.dot_general(low, fold, (((0,), (0,)), ((), ())), preferred_element_type=F32)
    group = 4 if n_tok % 4 == 0 else 1
    delta = None
    for g in range(0, n_tok, group):
        chosen = jnp.concatenate(
            [
                jnp.where(wanted[...] == b * adp_dev, spread, 0.0).astype(BF16)
                for b in range(g, g + group)
            ],
            axis=1,
        )
        weights = ups[g : g + group].reshape(group * lanes, kv)
        term = jnp.dot(chosen, weights, preferred_element_type=F32)
        delta = term if delta is None else delta + term
    out_ref[...] = (partial[x] + delta.astype(BF16).astype(F32)).astype(BF16)

    to_hid(1, h, low_recv.at[pl.ds(0, n_hid - 1)]).wait_send()
    for d in range(chips):
        to_core(d).wait_send()
    for d in range(1, chips):
        to_chip(d, x).wait_send()

    half = downs.at[0, pl.ds(0, CHUNKS)]
    short = downs.at[0, pl.ds(0, CHUNKS - EXTRA // SPLIT)]
    single = downs.at[0, pl.ds(0, EXTRA // SPLIT)]

    @pl.when(z < last)
    def _():
        to_right(0, PIECES, single).wait_send()

    @pl.when(z > 0)
    def _():
        to_left(last, PIECES, single).wait_send()

    def drain(block, carry):
        @pl.when((block <= z) & (z < last))
        def _():
            to_right(block, 0, half).wait_send()
            to_right(block, UP).wait_send()

        @pl.when((block >= z) & (z > 0))
        def _():
            to_left(block, 0, half).wait_send()
            to_left(block, UP).wait_send()

        end = (block == 0) | (block == last)

        @pl.when((block != z) & end)
        def _():
            to_pair(block, y, 0, short).wait_send()

        @pl.when((block != z) & ~end)
        def _():
            to_pair(block, y, 0, half).wait_send()

        return carry

    lax.fori_loop(0, n_tok, drain, 0)


def per_device(n_tok, n_hid, tokens, adapter_ids, value_weight, adapter_down, adapter_up):
    rows, depth = tokens.shape
    adp_dev, rank, kv = adapter_up.shape
    lanes = adp_dev * rank
    chips = n_hid // 2
    hbm = pl.BlockSpec(memory_space=pltpu.HBM)
    dma = pltpu.SemaphoreType.DMA
    return pl.pallas_call(
        functools.partial(kernel, n_tok, n_hid, rank),
        out_shape=pltpu.VMEM((rows, kv), BF16),
        in_specs=[hbm] * 5,
        out_specs=pl.BlockSpec(memory_space=pltpu.VMEM),
        scratch_shapes=[
            pltpu.VMEM((1, rows), jnp.int32),
            pltpu.VMEM((rows, depth), BF16),
            pltpu.VMEM((2 * chips, depth, kv), BF16),
            pltpu.VMEM((n_tok, 2 * CHUNKS, lanes, depth // (2 * CHUNKS)), BF16),
            pltpu.VMEM((n_tok, lanes, kv), BF16),
            pltpu.VMEM((chips, rows, kv), BF16),
            pltpu.VMEM((chips, rows, kv), BF16),
            pltpu.VMEM((chips, rows, kv), F32),
            pltpu.VMEM((chips, rows, kv), BF16),
            pltpu.VMEM((chips, rows, kv), BF16),
            pltpu.VMEM((rows, lanes), F32),
            pltpu.VMEM((rows, lanes), jnp.int32),
            pltpu.VMEM((rank, rows), BF16),
            pltpu.VMEM((n_hid, rank, rows), BF16),
            dma((5,)),
            dma((2 * n_tok + 1,)),
            dma((2 * n_tok + 1,)),
            dma((n_tok - 1, PIECES + 1)),
            dma((2, EXTRA)),
            dma((n_tok,)),
            dma((n_tok - 1, CHUNKS)),
            dma((chips,)),
            dma((chips,)),
            dma((chips,)),
            dma((chips,)),
            dma,
            dma((n_hid,)),
            pltpu.SemaphoreType.REGULAR,
        ],
        compiler_params=pltpu.CompilerParams(
            collective_id=0, has_side_effects=True, vmem_limit_bytes=60 * 1024 * 1024
        ),
    )(
        adapter_ids.reshape(1, rows),
        tokens,
        value_weight,
        adapter_down.reshape(lanes, depth),
        adapter_up.reshape(lanes, kv),
    )


def solution(mesh):
    in_specs = (
        P(("parts", "tok"), "hid"),
        P(("parts", "tok"), None),
        P("hid", None),
        P("tok", None, "hid"),
        P("tok", None, "hid"),
    )
    out_specs = P(("parts", "tok"), "hid")
    body = functools.partial(per_device, mesh.shape["tok"], mesh.shape["hid"])
    return jax.shard_map(body, mesh=mesh, in_specs=in_specs, out_specs=out_specs, check_vma=False)
```

```python
import functools

import jax
import jax.numpy as jnp
from jax import lax
from jax.experimental import pallas as pl
from jax.experimental.pallas import tpu as pltpu
from jax.sharding import PartitionSpec as P

MESH = pl.DeviceIdType.MESH
F32 = jnp.float32
BF16 = jnp.bfloat16

CHUNKS = 4
SPLIT = 2
PIECES = CHUNKS * SPLIT
EXTRA = 2
UP = PIECES + EXTRA


def kernel(
    n_tok,
    n_hid,
    rank,
    ids_hbm,
    tokens_hbm,
    value_hbm,
    down_hbm,
    up_hbm,
    out_ref,
    ids,
    tokens,
    value,
    downs,
    ups,
    core_send,
    core_recv,
    partial,
    chip_send,
    chip_recv,
    spare,
    picked,
    wanted,
    low_send,
    low_recv,
    load_sem,
    right_sem,
    left_sem,
    line_sem,
    extra_sem,
    pair_send_sem,
    pair_recv_sem,
    core_send_sem,
    core_recv_sem,
    chip_send_sem,
    chip_recv_sem,
    low_send_sem,
    low_recv_sem,
    ready_sem,
):
    y = lax.axis_index("parts")
    z = lax.axis_index("tok")
    h = lax.axis_index("hid")
    chips = n_hid // 2
    core = lax.rem(h, 2)
    x = lax.div(h, 2)
    rows, depth = tokens.shape
    kv = out_ref.shape[1]
    lanes, width = downs.shape[2:]
    adp_dev = lanes // rank
    part = lanes // SPLIT
    last = n_tok - 1

    load_down = [
        pltpu.make_async_copy(
            down_hbm.at[:, pl.ds(p * width, width)], downs.at[z, p], load_sem.at[3]
        )
        for p in range(2 * CHUNKS)
    ]
    chip_of = [lax.rem(x + d, chips) for d in range(chips)]
    order = [*range(1, chips), 0]
    columns_of = [(d, side) for d in order for side in (1, 0)]
    load_value = [
        pltpu.make_async_copy(
            value_hbm.at[
                :,
                pl.ds(
                    pl.multiple_of((chip_of[d] * 2 + (1 - core if side else core)) * kv, kv), kv
                ),
            ],
            value.at[k],
            load_sem.at[4 if k < 2 * (chips - 1) else 5],
        )
        for k, (d, side) in enumerate(columns_of)
    ]
    load_up = pltpu.make_async_copy(up_hbm, ups.at[z], load_sem.at[0])
    load_ids = pltpu.make_async_copy(ids_hbm, ids, load_sem.at[1])
    load_tokens = pltpu.make_async_copy(tokens_hbm, tokens, load_sem.at[2])
    for load in load_down:
        load.start()

    barrier = pltpu.get_barrier_semaphore()
    pl.semaphore_signal(barrier, inc=1, device_id={"parts": 1 - y}, device_id_type=MESH)
    for d in range(1, n_hid):
        pl.semaphore_signal(
            barrier, inc=1, device_id={"hid": lax.rem(h + d, n_hid)}, device_id_type=MESH
        )

    @pl.when(z < last)
    def _():
        pl.semaphore_signal(barrier, inc=1, device_id={"tok": z + 1}, device_id_type=MESH)

    pltpu.make_async_copy(downs.at[z], downs.at[z], load_sem.at[3]).wait()
    load_tokens.start()
    for load in load_value:
        load.start()
    load_up.start()
    load_ids.start()

    pl.semaphore_wait(barrier, n_hid + (z > 0).astype(jnp.int32))

    def piece(block, side, c):
        return downs.at[block, side * CHUNKS + c // SPLIT, pl.ds(c % SPLIT * part, part)]

    def line_piece(block, c):
        if c == UP:
            return ups.at[block]
        return piece(block, y, c) if c < PIECES else piece(block, 1 - y, c - EXTRA)

    def send_index(block, c):
        if c == UP:
            return n_tok + block
        return block if c < PIECES else 2 * n_tok

    def recv_sem(block, side, c):
        if PIECES <= c < UP:
            return extra_sem.at[side, c - PIECES]
        return line_sem.at[block - side, min(c, PIECES)]

    def to_right(block, c, ref=None):
        ref = line_piece(block, c) if ref is None else ref
        return pltpu.make_async_remote_copy(
            src_ref=ref,
            dst_ref=ref,
            send_sem=right_sem.at[send_index(block, c)],
            recv_sem=recv_sem(block, 0, c),
            device_id={"tok": z + 1},
            device_id_type=MESH,
        )

    def to_left(block, c, ref=None):
        ref = line_piece(block, c) if ref is None else ref
        return pltpu.make_async_remote_copy(
            src_ref=ref,
            dst_ref=ref,
            send_sem=left_sem.at[send_index(block, c)],
            recv_sem=recv_sem(block, 1, c),
            device_id={"tok": z - 1},
            device_id_type=MESH,
        )

    def to_pair(block, side, c, ref=None):
        ref = piece(block, side, c) if ref is None else ref
        return pltpu.make_async_remote_copy(
            src_ref=ref,
            dst_ref=ref,
            send_sem=pair_send_sem.at[block],
            recv_sem=pair_recv_sem.at[block - (block > z).astype(jnp.int32), c // SPLIT],
            device_id={"parts": 1 - y},
            device_id_type=MESH,
        )

    def wait_pair(block, c):
        count = [by_pair(0, k) is True for k in range(c * SPLIT, (c + 1) * SPLIT)].count(True)
        ref = downs.at[block, (1 - y) * CHUNKS + c]

        @pl.when((block != 0) & (block != last))
        def _():
            to_pair(block, 1 - y, c * SPLIT, ref).wait_recv()

        if count:
            @pl.when((block == 0) | (block == last))
            def _():
                to_pair(block, 1 - y, c * SPLIT, ref.at[pl.ds(0, count * part)]).wait_recv()

    @pl.when(z > 0)
    def _():
        pl.semaphore_signal(ready_sem, inc=1, device_id={"tok": z - 1}, device_id_type=MESH)
        for c in range(PIECES):
            to_left(z, c).start()

    @pl.when(z == last)
    def _():
        for c in range(PIECES, PIECES + EXTRA):
            to_left(z, c).start()

    def send_right():
        pl.semaphore_wait(ready_sem, 1)
        for c in range(PIECES):
            to_right(z, c).start()

        @pl.when(z == 0)
        def _():
            for c in range(PIECES, PIECES + EXTRA):
                to_right(z, c).start()

    def by_pair(block, c):
        return c < PIECES - EXTRA or (block != 0) & (block != last)

    def forward(s, first, end):
        from_left = z - 1 - s
        from_right = z + 1 + s
        for c in range(first, end):
            @pl.when(from_left >= 0 if c < PIECES else from_left == 0)
            def _():
                to_right(from_left, c).wait_recv()

                @pl.when(z < last)
                def _():
                    to_right(from_left, c).start()

                if c < PIECES:
                    @pl.when(by_pair(from_left, c))
                    def _():
                        to_pair(from_left, y, c).start()

            @pl.when(from_right <= last if c < PIECES else from_right == last)
            def _():
                to_left(from_right, c).wait_recv()

                @pl.when(z > 0)
                def _():
                    to_left(from_right, c).start()

                if c < PIECES:
                    @pl.when(by_pair(from_right, c))
                    def _():
                        to_pair(from_right, y, c).start()

    def forward_up(s):
        from_left = z - 1 - s
        from_right = z + 1 + s

        @pl.when((from_left >= 0) & (z < last))
        def _():
            to_right(from_left, UP).wait_recv()

            @pl.when((z < last - 1) | (s == n_tok - 3))
            def _():
                to_right(from_left, UP).start()

        @pl.when((from_right <= last) & (z > 0))
        def _():
            to_left(from_right, UP).wait_recv()

            @pl.when((z > 1) | (s == n_tok - 3))
            def _():
                to_left(from_right, UP).start()

    def flush_up():
        def send(block, carry):
            @pl.when(z == 1)
            def _():
                to_left(block, UP).start()

            @pl.when(z == last - 1)
            def _():
                to_right(block, UP).start()

            return carry

        lax.fori_loop(1, last, send, 0)

    alone = pl.when(z < n_tok)

    def base_block(k):
        return jnp.dot(tokens[...], value[k], preferred_element_type=F32)

    def to_core(d):
        return pltpu.make_async_remote_copy(
            src_ref=core_send.at[chip_of[d]],
            dst_ref=core_recv.at[chip_of[d]],
            send_sem=core_send_sem.at[d],
            recv_sem=core_recv_sem.at[d],
            device_id={"hid": x * 2 + 1 - core},
            device_id_type=MESH,
        )

    def to_chip(d, slot):
        i = chip_of[d]
        return pltpu.make_async_remote_copy(
            src_ref=chip_send.at[i],
            dst_ref=chip_recv.at[slot],
            send_sem=chip_send_sem.at[i],
            recv_sem=chip_recv_sem.at[slot],
            device_id={"hid": i * 2 + core},
            device_id_type=MESH,
        )

    pl.when((z > 0) & (z < last))(send_right)
    load_tokens.wait()
    others = value.at[pl.ds(0, 2 * (chips - 1))]
    pltpu.make_async_copy(others, others, load_sem.at[4]).wait()
    for n, d in enumerate(order[:-1]):
        i = chip_of[d]

        @alone
        def _():
            core_send[i] = base_block(2 * n).astype(BF16)

        to_core(d).start()
        if n == 0:
            pl.when(z == 0)(send_right)
            load_up.wait()

            @pl.when(z > 1)
            def _():
                to_left(z, UP).start()

            @pl.when(z < last - 1)
            def _():
                to_right(z, UP).start()

        @alone
        def _():
            partial[i] = base_block(2 * n + 1)

        to_core(d).wait_recv()
        chip_send[i] = (partial[i] + core_recv[i].astype(F32)).astype(BF16)
        to_chip(d, x).start()

    mine = value.at[pl.ds(2 * (chips - 1), 2)]
    pltpu.make_async_copy(mine, mine, load_sem.at[5]).wait()
    load_ids.wait()
    lane_adapter = lax.broadcasted_iota(jnp.int32, (rows, lanes), 1) // rank
    ids_rows = jnp.transpose(jnp.broadcast_to(ids[...], (lanes, rows)))
    wanted[...] = ids_rows - lane_adapter

    def low_part(block, p):
        columns = pl.ds(pl.multiple_of(p * width, width), width)
        return lax.dot_general(
            tokens[:, columns],
            downs[block, p],
            (((1,), (1,)), ((), ())),
            preferred_element_type=F32,
        )

    def chosen_of(block, sums):
        return jnp.where(wanted[...] == block * adp_dev, sums, 0.0)

    def low_block(block):
        return lax.dot_general(
            tokens[...],
            jnp.concatenate([downs[block, p] for p in range(2 * CHUNKS)], axis=1),
            (((1,), (1,)), ((), ())),
            preferred_element_type=F32,
        )

    def base_part(k, q):
        columns = slice(q * 2 * width, (q + 1) * 2 * width)
        return jnp.dot(tokens[:, columns], value[k, columns, :], preferred_element_type=F32)

    def pair_sum(q):
        sums = base_part(2 * (chips - 1), q)
        if q > 0:
            sums += spare[...]
        if q < CHUNKS - 1:
            spare[...] = sums
        else:
            core_send[x] = sums.astype(BF16)

    def own_sum(q):
        sums = base_part(2 * chips - 1, q)
        partial[x] = sums if q == 0 else partial[x] + sums

    def own_low(q):
        sums = low_part(z, 2 * q) + low_part(z, 2 * q + 1)
        sums = chosen_of(z, sums)
        picked[...] = sums if q == 0 else picked[...] + sums

    work = [
        functools.partial(part_of, q)
        for part_of in (pair_sum, own_sum, own_low)
        for q in range(CHUNKS)
    ]
    done = 0
    for c in range(PIECES):
        forward(0, c, c + 1)
        upto = len(work) * (c + 1) // PIECES
        for k in range(done, upto):
            alone(work[k])
            if k == CHUNKS - 1:
                to_core(0).start()
        done = upto
    forward(0, PIECES, PIECES + EXTRA)

    def low_chunk(s, c):
        for at, block in ((last, last - 1 - s), (0, 1 + s)):
            @pl.when(z == at)
            def _():
                wait_pair(block, c)
                sums = low_part(block, y * CHUNKS + c) + low_part(block, (1 - y) * CHUNKS + c)
                picked[...] += chosen_of(block, sums)

    def low_whole(s, carry):
        for sign in (-1, 1):
            block = z + sign * (1 + s)

            @pl.when((block >= 0) & (block <= last))
            def _():
                for c in range(CHUNKS):
                    wait_pair(block, c)

                picked[...] += chosen_of(block, low_block(block))

        return carry

    def step(s, carry=0):
        for c in range(CHUNKS):
            forward(s, c * SPLIT, (c + 1) * SPLIT)
            if c == 1:
                forward_up(s - 1)
            low_chunk(s - 1, c)
        forward(s, PIECES, PIECES + EXTRA)
        return carry

    if n_tok <= 8:
        for s in range(1, n_tok - 2):
            step(s)
    else:
        lax.fori_loop(1, n_tok - 2, step, 0)
    flush_up()

    s = n_tok - 2
    for c in range(CHUNKS):
        forward(s, c * SPLIT, (c + 1) * SPLIT)
        if c == 1:
            forward_up(s - 1)
        if c < CHUNKS - 1:
            low_chunk(s - 1, c)
        if c == CHUNKS - 2:
            low_chunk(s - 1, CHUNKS - 1)
    low_chunk(s, 0)

    to_core(0).wait_recv()
    total = partial[x] + core_recv[x].astype(F32)
    for d in range(1, chips):
        to_chip(d, chip_of[d]).wait_recv()
        total += chip_recv[chip_of[d]].astype(F32)
    partial[x] = total

    forward(s, PIECES, PIECES + EXTRA)
    for c in range(1, CHUNKS - 2):
        low_chunk(s, c)
    low_chunk(s, CHUNKS - 1)
    low_chunk(s, CHUNKS - 2)

    @pl.when((z > 0) & (z < last))
    def _():
        lax.fori_loop(0, last - 1, low_whole, 0)

    fold = (
        lax.rem(lax.broadcasted_iota(jnp.int32, (rank, lanes), 1), rank)
        == lax.broadcasted_iota(jnp.int32, (rank, lanes), 0)
    ).astype(F32).astype(BF16)
    low_send[...] = lax.dot_general(
        fold,
        picked[...].astype(BF16),
        (((1,), (1,)), ((), ())),
        preferred_element_type=F32,
    ).astype(BF16)

    def to_hid(d, slot, ref=None):
        return pltpu.make_async_remote_copy(
            src_ref=low_send if ref is None else ref,
            dst_ref=low_recv.at[slot] if ref is None else ref,
            send_sem=low_send_sem,
            recv_sem=low_recv_sem.at[slot],
            device_id={"hid": lax.rem(h + d, n_hid)},
            device_id_type=MESH,
        )

    for d in range(1, n_hid):
        to_hid(d, h).start()

    def late_up(block, carry):
        @pl.when((z == 0) & (block > 0))
        def _():
            to_left(block, UP).wait_recv()

        @pl.when((z == last) & (block < last))
        def _():
            to_right(block, UP).wait_recv()

        return carry

    lax.fori_loop(0, n_tok, late_up, 0)

    low = low_send[...].astype(F32)
    for d in range(1, n_hid):
        slot = lax.rem(h + d, n_hid)
        to_hid(d, slot).wait_recv()
        low += low_recv[slot].astype(F32)
    low = low.astype(BF16)

    spread = lax.dot_general(low, fold, (((0,), (0,)), ((), ())), preferred_element_type=F32)
    group = 4 if n_tok % 4 == 0 else 1
    delta = None
    for g in range(0, n_tok, group):
        chosen = jnp.concatenate(
            [
                jnp.where(wanted[...] == b * adp_dev, spread, 0.0).astype(BF16)
                for b in range(g, g + group)
            ],
            axis=1,
        )
        weights = ups[g : g + group].reshape(group * lanes, kv)
        term = jnp.dot(chosen, weights, preferred_element_type=F32)
        delta = term if delta is None else delta + term
    out_ref[...] = (partial[x] + delta.astype(BF16).astype(F32)).astype(BF16)

    to_hid(1, h, low_recv.at[pl.ds(0, n_hid - 1)]).wait_send()
    for d in range(chips):
        to_core(d).wait_send()
    for d in range(1, chips):
        to_chip(d, x).wait_send()

    half = downs.at[0, pl.ds(0, PIECES), pl.ds(0, part)]
    short = downs.at[0, pl.ds(0, PIECES - EXTRA), pl.ds(0, part)]
    single = downs.at[0, pl.ds(0, EXTRA), pl.ds(0, part)]

    @pl.when(z < last)
    def _():
        to_right(0, PIECES, single).wait_send()

    @pl.when(z > 0)
    def _():
        to_left(last, PIECES, single).wait_send()

    def drain(block, carry):
        @pl.when((block <= z) & (z < last))
        def _():
            to_right(block, 0, half).wait_send()
            to_right(block, UP).wait_send()

        @pl.when((block >= z) & (z > 0))
        def _():
            to_left(block, 0, half).wait_send()
            to_left(block, UP).wait_send()

        end = (block == 0) | (block == last)

        @pl.when((block != z) & end)
        def _():
            to_pair(block, y, 0, short).wait_send()

        @pl.when((block != z) & ~end)
        def _():
            to_pair(block, y, 0, half).wait_send()

        return carry

    lax.fori_loop(0, n_tok, drain, 0)


def per_device(n_tok, n_hid, tokens, adapter_ids, value_weight, adapter_down, adapter_up):
    rows, depth = tokens.shape
    adp_dev, rank, kv = adapter_up.shape
    lanes = adp_dev * rank
    chips = n_hid // 2
    hbm = pl.BlockSpec(memory_space=pltpu.HBM)
    dma = pltpu.SemaphoreType.DMA
    return pl.pallas_call(
        functools.partial(kernel, n_tok, n_hid, rank),
        out_shape=pltpu.VMEM((rows, kv), BF16),
        in_specs=[hbm] * 5,
        out_specs=pl.BlockSpec(memory_space=pltpu.VMEM),
        scratch_shapes=[
            pltpu.VMEM((1, rows), jnp.int32),
            pltpu.VMEM((rows, depth), BF16),
            pltpu.VMEM((2 * chips, depth, kv), BF16),
            pltpu.VMEM((n_tok, 2 * CHUNKS, lanes, depth // (2 * CHUNKS)), BF16),
            pltpu.VMEM((n_tok, lanes, kv), BF16),
            pltpu.VMEM((chips, rows, kv), BF16),
            pltpu.VMEM((chips, rows, kv), BF16),
            pltpu.VMEM((chips, rows, kv), F32),
            pltpu.VMEM((chips, rows, kv), BF16),
            pltpu.VMEM((chips, rows, kv), BF16),
            pltpu.VMEM((rows, kv), F32),
            pltpu.VMEM((rows, lanes), F32),
            pltpu.VMEM((rows, lanes), jnp.int32),
            pltpu.VMEM((rank, rows), BF16),
            pltpu.VMEM((n_hid, rank, rows), BF16),
            dma((6,)),
            dma((2 * n_tok + 1,)),
            dma((2 * n_tok + 1,)),
            dma((n_tok - 1, PIECES + 1)),
            dma((2, EXTRA)),
            dma((n_tok,)),
            dma((n_tok - 1, CHUNKS)),
            dma((chips,)),
            dma((chips,)),
            dma((chips,)),
            dma((chips,)),
            dma,
            dma((n_hid,)),
            pltpu.SemaphoreType.REGULAR,
        ],
        compiler_params=pltpu.CompilerParams(
            collective_id=0, has_side_effects=True, vmem_limit_bytes=60 * 1024 * 1024
        ),
    )(
        adapter_ids.reshape(1, rows),
        tokens,
        value_weight,
        adapter_down.reshape(lanes, depth),
        adapter_up.reshape(lanes, kv),
    )


def solution(mesh):
    in_specs = (
        P(("parts", "tok"), "hid"),
        P(("parts", "tok"), None),
        P("hid", None),
        P("tok", None, "hid"),
        P("tok", None, "hid"),
    )
    out_specs = P(("parts", "tok"), "hid")
    body = functools.partial(per_device, mesh.shape["tok"], mesh.shape["hid"])
    return jax.shard_map(body, mesh=mesh, in_specs=in_specs, out_specs=out_specs, check_vma=False)
```

```python
import functools

import jax
import jax.numpy as jnp
from jax import lax
from jax.experimental import pallas as pl
from jax.experimental.pallas import tpu as pltpu
from jax.sharding import PartitionSpec as P

MESH = pl.DeviceIdType.MESH
F32 = jnp.float32
BF16 = jnp.bfloat16

CHUNKS = 4
SPLIT = 2
PIECES = CHUNKS * SPLIT
EXTRA = 2
UP = PIECES + EXTRA


def kernel(
    n_tok,
    n_hid,
    rank,
    ids_hbm,
    tokens_hbm,
    value_hbm,
    down_hbm,
    up_hbm,
    out_ref,
    ids,
    tokens,
    value,
    downs,
    ups,
    core_send,
    core_recv,
    partial,
    chip_send,
    chip_recv,
    spare,
    picked,
    wanted,
    low_send,
    low_recv,
    load_sem,
    right_sem,
    left_sem,
    line_sem,
    extra_sem,
    pair_send_sem,
    pair_recv_sem,
    core_send_sem,
    core_recv_sem,
    chip_send_sem,
    chip_recv_sem,
    low_send_sem,
    low_recv_sem,
    ready_sem,
):
    y = lax.axis_index("parts")
    z = lax.axis_index("tok")
    h = lax.axis_index("hid")
    chips = n_hid // 2
    core = lax.rem(h, 2)
    x = lax.div(h, 2)
    rows, depth = tokens.shape
    kv = out_ref.shape[1]
    lanes, width = downs.shape[2:]
    adp_dev = lanes // rank
    part = lanes // SPLIT
    last = n_tok - 1

    load_down = [
        pltpu.make_async_copy(
            down_hbm.at[:, pl.ds(p * width, width)], downs.at[z, p], load_sem.at[3]
        )
        for p in range(2 * CHUNKS)
    ]
    chip_of = [lax.rem(x + d, chips) for d in range(chips)]
    order = [*range(1, chips), 0]
    columns_of = [(d, side) for d in order for side in (1, 0)]
    load_value = [
        pltpu.make_async_copy(
            value_hbm.at[
                :,
                pl.ds(
                    pl.multiple_of((chip_of[d] * 2 + (1 - core if side else core)) * kv, kv), kv
                ),
            ],
            value.at[k],
            load_sem.at[4 if k < 2 * (chips - 1) else 5],
        )
        for k, (d, side) in enumerate(columns_of)
    ]
    load_up = pltpu.make_async_copy(up_hbm, ups.at[z], load_sem.at[0])
    load_ids = pltpu.make_async_copy(ids_hbm, ids, load_sem.at[1])
    load_tokens = pltpu.make_async_copy(tokens_hbm, tokens, load_sem.at[2])
    for load in load_down:
        load.start()

    barrier = pltpu.get_barrier_semaphore()
    pl.semaphore_signal(barrier, inc=1, device_id={"parts": 1 - y}, device_id_type=MESH)
    for d in range(1, n_hid):
        pl.semaphore_signal(
            barrier, inc=1, device_id={"hid": lax.rem(h + d, n_hid)}, device_id_type=MESH
        )

    @pl.when(z < last)
    def _():
        pl.semaphore_signal(barrier, inc=1, device_id={"tok": z + 1}, device_id_type=MESH)

    pltpu.make_async_copy(downs.at[z], downs.at[z], load_sem.at[3]).wait()
    load_tokens.start()
    for load in load_value:
        load.start()
    load_up.start()
    load_ids.start()

    pl.semaphore_wait(barrier, n_hid + (z > 0).astype(jnp.int32))

    def piece(block, side, c):
        return downs.at[block, side * CHUNKS + c // SPLIT, pl.ds(c % SPLIT * part, part)]

    def line_piece(block, c):
        if c == UP:
            return ups.at[block]
        return piece(block, y, c) if c < PIECES else piece(block, 1 - y, c - EXTRA)

    def send_index(block, c):
        if c == UP:
            return n_tok + block
        return block if c < PIECES else 2 * n_tok

    def recv_sem(block, side, c):
        if PIECES <= c < UP:
            return extra_sem.at[side, c - PIECES]
        return line_sem.at[block - side, min(c, PIECES)]

    def to_right(block, c, ref=None):
        ref = line_piece(block, c) if ref is None else ref
        return pltpu.make_async_remote_copy(
            src_ref=ref,
            dst_ref=ref,
            send_sem=right_sem.at[send_index(block, c)],
            recv_sem=recv_sem(block, 0, c),
            device_id={"tok": z + 1},
            device_id_type=MESH,
        )

    def to_left(block, c, ref=None):
        ref = line_piece(block, c) if ref is None else ref
        return pltpu.make_async_remote_copy(
            src_ref=ref,
            dst_ref=ref,
            send_sem=left_sem.at[send_index(block, c)],
            recv_sem=recv_sem(block, 1, c),
            device_id={"tok": z - 1},
            device_id_type=MESH,
        )

    def to_pair(block, side, c, ref=None):
        ref = piece(block, side, c) if ref is None else ref
        return pltpu.make_async_remote_copy(
            src_ref=ref,
            dst_ref=ref,
            send_sem=pair_send_sem.at[block],
            recv_sem=pair_recv_sem.at[block - (block > z).astype(jnp.int32), c // SPLIT],
            device_id={"parts": 1 - y},
            device_id_type=MESH,
        )

    def wait_pair(block, c):
        count = [by_pair(0, k) is True for k in range(c * SPLIT, (c + 1) * SPLIT)].count(True)
        ref = downs.at[block, (1 - y) * CHUNKS + c]

        @pl.when((block != 0) & (block != last))
        def _():
            to_pair(block, 1 - y, c * SPLIT, ref).wait_recv()

        if count:
            @pl.when((block == 0) | (block == last))
            def _():
                to_pair(block, 1 - y, c * SPLIT, ref.at[pl.ds(0, count * part)]).wait_recv()

    @pl.when(z > 0)
    def _():
        pl.semaphore_signal(ready_sem, inc=1, device_id={"tok": z - 1}, device_id_type=MESH)
        for c in range(PIECES):
            to_left(z, c).start()

    @pl.when(z == last)
    def _():
        for c in range(PIECES, PIECES + EXTRA):
            to_left(z, c).start()

    def send_right():
        pl.semaphore_wait(ready_sem, 1)
        for c in range(PIECES):
            to_right(z, c).start()

        @pl.when(z == 0)
        def _():
            for c in range(PIECES, PIECES + EXTRA):
                to_right(z, c).start()

    def by_pair(block, c):
        return c < PIECES - EXTRA or (block != 0) & (block != last)

    def forward(s, first, end):
        from_left = z - 1 - s
        from_right = z + 1 + s
        for c in range(first, end):
            @pl.when(from_left >= 0 if c < PIECES else from_left == 0)
            def _():
                to_right(from_left, c).wait_recv()

                @pl.when(z < last)
                def _():
                    to_right(from_left, c).start()

                if c < PIECES:
                    @pl.when(by_pair(from_left, c))
                    def _():
                        to_pair(from_left, y, c).start()

            @pl.when(from_right <= last if c < PIECES else from_right == last)
            def _():
                to_left(from_right, c).wait_recv()

                @pl.when(z > 0)
                def _():
                    to_left(from_right, c).start()

                if c < PIECES:
                    @pl.when(by_pair(from_right, c))
                    def _():
                        to_pair(from_right, y, c).start()

    def forward_up(s):
        from_left = z - 1 - s
        from_right = z + 1 + s

        @pl.when((from_left >= 0) & (z < last))
        def _():
            to_right(from_left, UP).wait_recv()

            @pl.when((z < last - 1) | (s == n_tok - 3))
            def _():
                to_right(from_left, UP).start()

        @pl.when((from_right <= last) & (z > 0))
        def _():
            to_left(from_right, UP).wait_recv()

            @pl.when((z > 1) | (s == n_tok - 3))
            def _():
                to_left(from_right, UP).start()

    def flush_up():
        def send(block, carry):
            @pl.when(z == 1)
            def _():
                to_left(block, UP).start()

            @pl.when(z == last - 1)
            def _():
                to_right(block, UP).start()

            return carry

        lax.fori_loop(1, last, send, 0)

    alone = pl.when(z < n_tok)

    def base_block(k):
        return jnp.dot(tokens[...], value[k], preferred_element_type=F32)

    def to_core(d):
        return pltpu.make_async_remote_copy(
            src_ref=core_send.at[chip_of[d]],
            dst_ref=core_recv.at[chip_of[d]],
            send_sem=core_send_sem.at[d],
            recv_sem=core_recv_sem.at[d],
            device_id={"hid": x * 2 + 1 - core},
            device_id_type=MESH,
        )

    def to_chip(d, slot):
        i = chip_of[d]
        return pltpu.make_async_remote_copy(
            src_ref=chip_send.at[i],
            dst_ref=chip_recv.at[slot],
            send_sem=chip_send_sem.at[i],
            recv_sem=chip_recv_sem.at[slot],
            device_id={"hid": i * 2 + core},
            device_id_type=MESH,
        )

    pl.when((z > 0) & (z < last))(send_right)
    load_tokens.wait()
    others = value.at[pl.ds(0, 2 * (chips - 1))]
    pltpu.make_async_copy(others, others, load_sem.at[4]).wait()
    for n, d in enumerate(order[:-1]):
        i = chip_of[d]

        @alone
        def _():
            core_send[i] = base_block(2 * n).astype(BF16)

        to_core(d).start()
        if n == 0:
            pl.when(z == 0)(send_right)
            load_up.wait()

            @pl.when(z > 1)
            def _():
                to_left(z, UP).start()

            @pl.when(z < last - 1)
            def _():
                to_right(z, UP).start()

        @alone
        def _():
            partial[i] = base_block(2 * n + 1)

        to_core(d).wait_recv()
        chip_send[i] = (partial[i] + core_recv[i].astype(F32)).astype(BF16)
        to_chip(d, x).start()

    mine = value.at[pl.ds(2 * (chips - 1), 2)]
    pltpu.make_async_copy(mine, mine, load_sem.at[5]).wait()
    load_ids.wait()
    lane_adapter = lax.broadcasted_iota(jnp.int32, (rows, lanes), 1) // rank
    ids_rows = jnp.transpose(jnp.broadcast_to(ids[...], (lanes, rows)))
    wanted[...] = ids_rows - lane_adapter

    def low_part(block, p):
        columns = pl.ds(pl.multiple_of(p * width, width), width)
        return lax.dot_general(
            tokens[:, columns],
            downs[block, p],
            (((1,), (1,)), ((), ())),
            preferred_element_type=F32,
        )

    def chosen_of(block, sums):
        return jnp.where(wanted[...] == block * adp_dev, sums, 0.0)

    def low_block(block):
        return lax.dot_general(
            tokens[...],
            jnp.concatenate([downs[block, p] for p in range(2 * CHUNKS)], axis=1),
            (((1,), (1,)), ((), ())),
            preferred_element_type=F32,
        )

    def base_part(k, q):
        columns = slice(q * 2 * width, (q + 1) * 2 * width)
        return jnp.dot(tokens[:, columns], value[k, columns, :], preferred_element_type=F32)

    def pair_sum(q):
        sums = base_part(2 * (chips - 1), q)
        if q > 0:
            sums += spare[...]
        if q < CHUNKS - 1:
            spare[...] = sums
        else:
            core_send[x] = sums.astype(BF16)

    def own_sum(q):
        sums = base_part(2 * chips - 1, q)
        partial[x] = sums if q == 0 else partial[x] + sums

    def own_low(q):
        sums = low_part(z, 2 * q) + low_part(z, 2 * q + 1)
        sums = chosen_of(z, sums)
        picked[...] = sums if q == 0 else picked[...] + sums

    work = [
        functools.partial(part_of, q)
        for part_of in (pair_sum, own_sum, own_low)
        for q in range(CHUNKS)
    ]
    done = 0
    for c in range(PIECES):
        forward(0, c, c + 1)
        upto = len(work) * (c + 1) // PIECES
        for k in range(done, upto):
            alone(work[k])
            if k == CHUNKS - 1:
                to_core(0).start()
        done = upto
    forward(0, PIECES, PIECES + EXTRA)

    def low_chunk(s, c, sides=(0, 1)):
        for at, block in ((last, last - 1 - s), (0, 1 + s)):
            @pl.when(z == at)
            def _():
                if 1 in sides:
                    wait_pair(block, c)
                sums = [low_part(block, (y if side == 0 else 1 - y) * CHUNKS + c) for side in sides]
                picked[...] += chosen_of(block, sum(sums[1:], sums[0]))

    def low_whole(s, carry):
        for sign in (-1, 1):
            block = z + sign * (1 + s)

            @pl.when((block >= 0) & (block <= last))
            def _():
                for c in range(CHUNKS):
                    wait_pair(block, c)

                picked[...] += chosen_of(block, low_block(block))

        return carry

    def step(s, carry=0):
        for c in range(CHUNKS):
            forward(s, c * SPLIT, c * SPLIT + 1)
            low_chunk(s - 1, c, (0,))
            forward(s, c * SPLIT + 1, (c + 1) * SPLIT)
            if c == 1:
                forward_up(s - 1)
            low_chunk(s - 1, c, (1,))
        forward(s, PIECES, PIECES + EXTRA)
        return carry

    if n_tok <= 8:
        for s in range(1, n_tok - 2):
            step(s)
    else:
        lax.fori_loop(1, n_tok - 2, step, 0)
    flush_up()

    s = n_tok - 2
    for c in range(CHUNKS):
        forward(s, c * SPLIT, c * SPLIT + 1)
        if c < CHUNKS - 1:
            low_chunk(s - 1, c, (0,))
        forward(s, c * SPLIT + 1, (c + 1) * SPLIT)
        if c == 1:
            forward_up(s - 1)
        if c < CHUNKS - 1:
            low_chunk(s - 1, c, (1,))
        if c == CHUNKS - 2:
            low_chunk(s - 1, CHUNKS - 1)
    low_chunk(s, 0)

    to_core(0).wait_recv()
    total = partial[x] + core_recv[x].astype(F32)
    for d in range(1, chips):
        to_chip(d, chip_of[d]).wait_recv()
        total += chip_recv[chip_of[d]].astype(F32)
    partial[x] = total

    forward(s, PIECES, PIECES + EXTRA)
    for c in range(1, CHUNKS - 2):
        low_chunk(s, c)
    low_chunk(s, CHUNKS - 2, (0,))
    low_chunk(s, CHUNKS - 1)
    low_chunk(s, CHUNKS - 2, (1,))

    @pl.when((z > 0) & (z < last))
    def _():
        lax.fori_loop(0, last - 1, low_whole, 0)

    fold = (
        lax.rem(lax.broadcasted_iota(jnp.int32, (rank, lanes), 1), rank)
        == lax.broadcasted_iota(jnp.int32, (rank, lanes), 0)
    ).astype(F32).astype(BF16)
    low_send[...] = lax.dot_general(
        fold,
        picked[...].astype(BF16),
        (((1,), (1,)), ((), ())),
        preferred_element_type=F32,
    ).astype(BF16)

    def to_hid(d, slot, ref=None):
        return pltpu.make_async_remote_copy(
            src_ref=low_send if ref is None else ref,
            dst_ref=low_recv.at[slot] if ref is None else ref,
            send_sem=low_send_sem,
            recv_sem=low_recv_sem.at[slot],
            device_id={"hid": lax.rem(h + d, n_hid)},
            device_id_type=MESH,
        )

    for d in range(1, n_hid):
        to_hid(d, h).start()

    def late_up(block, carry):
        @pl.when((z == 0) & (block > 0))
        def _():
            to_left(block, UP).wait_recv()

        @pl.when((z == last) & (block < last))
        def _():
            to_right(block, UP).wait_recv()

        return carry

    lax.fori_loop(0, n_tok, late_up, 0)

    low = low_send[...].astype(F32)
    for d in range(1, n_hid):
        slot = lax.rem(h + d, n_hid)
        to_hid(d, slot).wait_recv()
        low += low_recv[slot].astype(F32)
    low = low.astype(BF16)

    spread = lax.dot_general(low, fold, (((0,), (0,)), ((), ())), preferred_element_type=F32)
    group = 4 if n_tok % 4 == 0 else 1
    delta = None
    for g in range(0, n_tok, group):
        chosen = jnp.concatenate(
            [
                jnp.where(wanted[...] == b * adp_dev, spread, 0.0).astype(BF16)
                for b in range(g, g + group)
            ],
            axis=1,
        )
        weights = ups[g : g + group].reshape(group * lanes, kv)
        term = jnp.dot(chosen, weights, preferred_element_type=F32)
        delta = term if delta is None else delta + term
    out_ref[...] = (partial[x] + delta.astype(BF16).astype(F32)).astype(BF16)

    to_hid(1, h, low_recv.at[pl.ds(0, n_hid - 1)]).wait_send()
    for d in range(chips):
        to_core(d).wait_send()
    for d in range(1, chips):
        to_chip(d, x).wait_send()

    half = downs.at[0, pl.ds(0, PIECES), pl.ds(0, part)]
    short = downs.at[0, pl.ds(0, PIECES - EXTRA), pl.ds(0, part)]
    single = downs.at[0, pl.ds(0, EXTRA), pl.ds(0, part)]

    @pl.when(z < last)
    def _():
        to_right(0, PIECES, single).wait_send()

    @pl.when(z > 0)
    def _():
        to_left(last, PIECES, single).wait_send()

    def drain(block, carry):
        @pl.when((block <= z) & (z < last))
        def _():
            to_right(block, 0, half).wait_send()
            to_right(block, UP).wait_send()

        @pl.when((block >= z) & (z > 0))
        def _():
            to_left(block, 0, half).wait_send()
            to_left(block, UP).wait_send()

        end = (block == 0) | (block == last)

        @pl.when((block != z) & end)
        def _():
            to_pair(block, y, 0, short).wait_send()

        @pl.when((block != z) & ~end)
        def _():
            to_pair(block, y, 0, half).wait_send()

        return carry

    lax.fori_loop(0, n_tok, drain, 0)


def per_device(n_tok, n_hid, tokens, adapter_ids, value_weight, adapter_down, adapter_up):
    rows, depth = tokens.shape
    adp_dev, rank, kv = adapter_up.shape
    lanes = adp_dev * rank
    chips = n_hid // 2
    hbm = pl.BlockSpec(memory_space=pltpu.HBM)
    dma = pltpu.SemaphoreType.DMA
    return pl.pallas_call(
        functools.partial(kernel, n_tok, n_hid, rank),
        out_shape=pltpu.VMEM((rows, kv), BF16),
        in_specs=[hbm] * 5,
        out_specs=pl.BlockSpec(memory_space=pltpu.VMEM),
        scratch_shapes=[
            pltpu.VMEM((1, rows), jnp.int32),
            pltpu.VMEM((rows, depth), BF16),
            pltpu.VMEM((2 * chips, depth, kv), BF16),
            pltpu.VMEM((n_tok, 2 * CHUNKS, lanes, depth // (2 * CHUNKS)), BF16),
            pltpu.VMEM((n_tok, lanes, kv), BF16),
            pltpu.VMEM((chips, rows, kv), BF16),
            pltpu.VMEM((chips, rows, kv), BF16),
            pltpu.VMEM((chips, rows, kv), F32),
            pltpu.VMEM((chips, rows, kv), BF16),
            pltpu.VMEM((chips, rows, kv), BF16),
            pltpu.VMEM((rows, kv), F32),
            pltpu.VMEM((rows, lanes), F32),
            pltpu.VMEM((rows, lanes), jnp.int32),
            pltpu.VMEM((rank, rows), BF16),
            pltpu.VMEM((n_hid, rank, rows), BF16),
            dma((6,)),
            dma((2 * n_tok + 1,)),
            dma((2 * n_tok + 1,)),
            dma((n_tok - 1, PIECES + 1)),
            dma((2, EXTRA)),
            dma((n_tok,)),
            dma((n_tok - 1, CHUNKS)),
            dma((chips,)),
            dma((chips,)),
            dma((chips,)),
            dma((chips,)),
            dma,
            dma((n_hid,)),
            pltpu.SemaphoreType.REGULAR,
        ],
        compiler_params=pltpu.CompilerParams(
            collective_id=0, has_side_effects=True, vmem_limit_bytes=60 * 1024 * 1024
        ),
    )(
        adapter_ids.reshape(1, rows),
        tokens,
        value_weight,
        adapter_down.reshape(lanes, depth),
        adapter_up.reshape(lanes, kv),
    )


def solution(mesh):
    in_specs = (
        P(("parts", "tok"), "hid"),
        P(("parts", "tok"), None),
        P("hid", None),
        P("tok", None, "hid"),
        P("tok", None, "hid"),
    )
    out_specs = P(("parts", "tok"), "hid")
    body = functools.partial(per_device, mesh.shape["tok"], mesh.shape["hid"])
    return jax.shard_map(body, mesh=mesh, in_specs=in_specs, out_specs=out_specs, check_vma=False)
```
